256 devices in a mesh: section: 8 (over z_lo, core), dp: 8 (over y, z_hi), tensor: 4 (over x).
Axes of the slice: x: 4, y: 4, z: 8 (z_hi: 2, z_lo: 4; z = z_hi * 4 + z_lo), core: 2. Of those that a mesh axis runs over, the one named last changes fastest.
Arguments:
- inputs: bfloat16 [32, 2, 64, 2560], P('dp', None, None, ('section', 'tensor')), parts along dimension 0, may hold values from -18 to 18
- sequence_jobs: int32 [32, 2, 1], P('dp'), parts along dimension 0, may hold values from 0 to 3
- entry_sequence: int32 [32], P('dp'), parts along dimension 0, may hold values from 0 to 3, each once
- layer_norm_gain: float32 [8, 2560], P('section'), may hold values from 0.25 to 1.75
- frozen_query_matrix: bfloat16 [8, 2560, 2560], P('section', None, 'tensor'), may hold values from -1 to 1
- frozen_key_matrix: bfloat16 [8, 2560, 2560], P('section', None, 'tensor'), may hold values from -24 to 24
- frozen_value_matrix: bfloat16 [8, 2560, 2560], P('section', None, 'tensor'), may hold values from -0.125 to 0.125
- frozen_output_matrix: bfloat16 [8, 2560, 2560], P('section', 'tensor'), may hold values from -0.125 to 0.125
- adapter_down_maps: bfloat16 [8, 2560, 128], P('section', 'tensor'), may hold values from -0.125 to 0.125
- adapter_up_maps: bfloat16 [8, 2, 64, 2560], P('section', None, None, 'tensor'), may hold values from -1.5 to 1.5
Outputs:
- finished: bfloat16 [32, 2, 64, 2560], P('dp', None, None, ('section', 'tensor')), parts along dimension 0
The draws below stay inside these ranges and needn't reach their ends.
There are 8 independent parts, one for each index of `dp`. The reference program is written for one: setup_inputs(seed, part) draws one part's arguments, and reference() takes and returns one part's arrays. A program takes and returns all parts, laid end to end along the dimension named above; an argument that names none is the same for every part. Nothing has to cross between parts.
Inputs may be any that keep to these rules, and one draw needn't show every extreme that they name: `sequence_jobs`: every one of the 4 jobs owns at least one sequence. `entry_sequence`: a permutation of the 4 micro-batches.
All inputs are finite; a program needn't handle non-finite values.
Results may differ from the reference program's by a relative error of at most 0.039.
Values may be sent and summed in bfloat16 or wider, within the bound.
A program may use at most 64 MiB of HBM per device.

```python
import math
import jax
import jax.numpy as jnp
from jax import lax

MODEL_WIDTH = 2560
HEADS = 20
HEAD_DIM = 128
ADAPTER_RANK = 16
ADAPTER_JOBS = 4
MICRO_SEQUENCES = 2
SEQ = 64
MICRO_BATCHES = 4
WINDOW_LAYERS = 8
N_TENSOR = 4


def shared_projection(key):
    base = jax.random.normal(jax.random.fold_in(key, 11), (WINDOW_LAYERS, MODEL_WIDTH, HEADS * HEAD_DIM), jnp.float32)
    return jnp.clip(base, -6.0, 6.0) / math.sqrt(MODEL_WIDTH)


def draw_frozen_query_matrix(key, part):
    return shared_projection(key).astype(jnp.bfloat16)


def draw_frozen_key_matrix(key, part):
    own_part = jax.random.normal(jax.random.fold_in(key, 12), (WINDOW_LAYERS, MODEL_WIDTH, HEADS * HEAD_DIM), jnp.float32)
    own_part = jnp.clip(own_part, -6.0, 6.0) / math.sqrt(MODEL_WIDTH)
    return own_part.astype(jnp.bfloat16)


def draw_inputs(key, part):
    full_shape = (MICRO_BATCHES, MICRO_SEQUENCES, SEQ, MODEL_WIDTH)
    base = jax.random.normal(jax.random.fold_in(key, 21), full_shape, jnp.float32)
    return jnp.clip(base, -6.0, 6.0).astype(jnp.bfloat16)


def block_levels(own_key, shape, split, least, high):
    def one(position, shards_of):
        draws = jax.random.uniform(jax.random.fold_in(jax.random.fold_in(own_key, 6), position), (shards_of,), jnp.float32, least / len(split), high / len(split))
        return jnp.repeat(jnp.exp(draws), shape[position] // shards_of).reshape((-1,) + (1,) * (len(shape) - position - 1))

    factor_of = one(*split[0])
    for cut in split[1:]:
        factor_of = factor_of * one(*cut)
    return factor_of


def different_ones(key, rows, number_of, top, lift):
    ranking = jax.random.permutation(jax.random.fold_in(key, 1), number_of)
    pull = ranking
    for power in range(3):
        pull = pull * pull // number_of
    pull = pull * lift // number_of
    tickets = jax.random.randint(jax.random.fold_in(key, 2), (rows, number_of), 0, 4096) + pull
    holders = jax.random.permutation(jax.random.fold_in(key, 3), rows)[jnp.arange(number_of) % rows]
    tickets = jnp.where(jnp.arange(rows)[:, None] == holders[None, :], 1 << 14, tickets)
    priority = tickets * number_of + jnp.arange(number_of)
    return lax.top_k(priority.astype(jnp.int32), top)[1].astype(jnp.int32)


def centred(rng, dims, scale, reach, pieces=(), held_as=jnp.bfloat16):
    factor_of = block_levels(rng, dims, pieces, -0.22, 0.18) if pieces else 1.0
    values = jax.random.normal(rng, dims, jnp.float32) * scale * factor_of
    return jnp.minimum(jnp.maximum(values, -reach), reach).astype(held_as)


def setup_inputs(seed: int = 0, part: int = 0) -> dict:
    seeds = jax.random.split(jax.random.key(seed), 11)
    own_keys = jax.random.split(jax.random.fold_in(seeds[10], part), 11)
    return {
        "inputs": draw_inputs(jax.random.fold_in(jax.random.fold_in(seeds[10], part), 71), part),
        "sequence_jobs": different_ones(own_keys[1], MICRO_BATCHES * MICRO_SEQUENCES, ADAPTER_JOBS, 1, 2048).reshape((MICRO_BATCHES, MICRO_SEQUENCES, 1)),
        "entry_sequence": jax.random.permutation(own_keys[2], MICRO_BATCHES).astype(jnp.int32),
        "layer_norm_gain": jnp.clip(1.0 + 0.15 * jax.random.normal(seeds[3], (WINDOW_LAYERS, MODEL_WIDTH), jnp.float32), 0.25, 1.75),
        "frozen_query_matrix": draw_frozen_query_matrix(jax.random.fold_in(seeds[10], 71), part),
        "frozen_key_matrix": draw_frozen_key_matrix(jax.random.fold_in(seeds[10], 71), part),
        "frozen_value_matrix": centred(seeds[6], (WINDOW_LAYERS, MODEL_WIDTH, MODEL_WIDTH), MODEL_WIDTH ** -0.5, 0.125, ((0, 8), (2, 4))),
        "frozen_output_matrix": centred(seeds[7], (WINDOW_LAYERS, MODEL_WIDTH, MODEL_WIDTH), MODEL_WIDTH ** -0.5, 0.125, ((0, 8), (1, 4))),
        "adapter_down_maps": centred(seeds[8], (WINDOW_LAYERS, MODEL_WIDTH, 2 * ADAPTER_JOBS * ADAPTER_RANK), MODEL_WIDTH ** -0.5, 0.125, ((0, 8), (1, 4))),
        "adapter_up_maps": centred(seeds[9], (WINDOW_LAYERS, 2, ADAPTER_JOBS * ADAPTER_RANK, MODEL_WIDTH), ADAPTER_RANK ** -0.5, 1.5, ((0, 8), (3, 4))),
    }


adapter_scale = 2.0

def attend(query_rows, key_vecs, value_rows, head_groupings):
    head_count = query_rows.shape[1] // HEAD_DIM
    grid_shape = (head_groupings, SEQ, head_count, HEAD_DIM)
    q_wide = query_rows.reshape(grid_shape).astype(jnp.float32)
    k_wide = key_vecs.reshape(grid_shape).astype(jnp.float32)
    v_wide = value_rows.reshape(grid_shape).astype(jnp.float32)
    scores = jnp.einsum('bqhd,bkhd->bhqk', q_wide, k_wide) * HEAD_DIM ** (-0.5)
    causal = jnp.arange(SEQ, dtype=jnp.int32)[:, None] >= jnp.arange(SEQ, dtype=jnp.int32)[None, :]
    scores = jnp.where(causal, scores, -jnp.inf)
    row_max = lax.optimization_barrier(jnp.max(scores, axis=-1, keepdims=True))
    weights = jnp.exp(scores - row_max)
    probabilities = (weights / lax.optimization_barrier(jnp.sum(weights, axis=-1, keepdims=True))).astype(jnp.bfloat16)
    mixture = jnp.einsum('bhqk,bkhd->bqhd', probabilities.astype(jnp.float32), v_wide)
    return mixture.astype(jnp.bfloat16).reshape(head_groupings * SEQ, head_count * HEAD_DIM)

def layer_forward(hidden_state, job_per_row, inverse_norm_scale, query_matrix, key_matrix, value_matrix, output_matrix, adapter_lower_part, adapter_upper_part, head_groupings):
    widened = hidden_state.astype(jnp.float32)
    meansq = lax.optimization_barrier(jnp.mean(widened * widened, axis=-1, keepdims=True))
    normalized_input = (widened * lax.rsqrt(meansq + 1e-05) * inverse_norm_scale).astype(jnp.bfloat16)
    lowrank_products = jnp.dot(normalized_input, adapter_lower_part, preferred_element_type=jnp.float32)
    column_job = jnp.arange(lowrank_products.shape[1], dtype=jnp.int32) // ADAPTER_RANK % ADAPTER_JOBS
    lowrank_products = jnp.where(column_job[None, :] == job_per_row[:, None], lowrank_products, 0.0).astype(jnp.bfloat16)
    middle_result = lowrank_products.shape[1] // 2
    query_rows = (jnp.dot(normalized_input, query_matrix, preferred_element_type=jnp.float32) + adapter_scale * jnp.dot(lowrank_products[:, :middle_result], adapter_upper_part[0], preferred_element_type=jnp.float32)).astype(jnp.bfloat16)
    key_vecs = jnp.dot(normalized_input, key_matrix, preferred_element_type=jnp.float32).astype(jnp.bfloat16)
    value_rows = (jnp.dot(normalized_input, value_matrix, preferred_element_type=jnp.float32) + adapter_scale * jnp.dot(lowrank_products[:, middle_result:], adapter_upper_part[1], preferred_element_type=jnp.float32)).astype(jnp.bfloat16)
    heads = attend(query_rows, key_vecs, value_rows, head_groupings)
    rows = heads.shape[0]
    block = MODEL_WIDTH // N_TENSOR
    head_blocks = heads.reshape(rows, N_TENSOR, block).astype(jnp.float32)
    weight_blocks = output_matrix.reshape(N_TENSOR, block, MODEL_WIDTH).astype(jnp.float32)
    partial_value = jnp.einsum('rbf,bfe->bre', head_blocks, weight_blocks).astype(jnp.bfloat16)
    partial_value = lax.optimization_barrier(partial_value)
    summed = lax.optimization_barrier(jnp.sum(partial_value.astype(jnp.float32), axis=0))
    return (widened + summed).astype(jnp.bfloat16)

def reference(inputs, sequence_jobs, entry_sequence, layer_norm_gain, frozen_query_matrix, frozen_key_matrix, frozen_value_matrix, frozen_output_matrix, adapter_down_maps, adapter_up_maps):
    ordered = jnp.take(inputs, entry_sequence, axis=0)
    seq_jobs = jnp.take(sequence_jobs, entry_sequence, axis=0)[:, :, 0]
    job_per_row = jnp.repeat(seq_jobs.reshape(-1), SEQ)
    hidden_state = ordered.reshape(MICRO_BATCHES * MICRO_SEQUENCES * SEQ, MODEL_WIDTH)
    for layer_number in range(WINDOW_LAYERS):
        hidden_state = layer_forward(hidden_state, job_per_row, layer_norm_gain[layer_number], frozen_query_matrix[layer_number], frozen_key_matrix[layer_number], frozen_value_matrix[layer_number], frozen_output_matrix[layer_number], adapter_down_maps[layer_number], adapter_up_maps[layer_number], MICRO_BATCHES * MICRO_SEQUENCES)
    return hidden_state.reshape(MICRO_BATCHES, MICRO_SEQUENCES, SEQ, MODEL_WIDTH)
```

```python
import functools

import jax
import jax.numpy as jnp
from jax import lax
from jax.experimental import pallas as pl
from jax.experimental.pallas import tpu as pltpu
from jax.sharding import PartitionSpec as P

HEAD_DIM = 128
ADAPTER_RANK = 16
ADAPTER_JOBS = 4
LANES = 128
MESH = pl.DeviceIdType.MESH
F32 = jnp.float32
BF16 = jnp.bfloat16


def relay_kernel(
    dims,
    xin_ref,
    mask_ref,
    gain_ref,
    up_ref,
    down_hbm,
    wq_hbm,
    wk_hbm,
    wv_hbm,
    wo_hbm,
    out_ref,
    wcat,
    wout,
    upcat,
    xbuf,
    acc,
    rs_out,
    rs_in,
    ag_out,
    ebuf,
    xout,
    w_sem,
    d_send,
    d_recv,
    e_send,
    e_recv,
    ea_send,
    x_recv,
    ag_send,
    rs_send,
    rs_recv,
    o_send,
    o_recv,
):
    S, T, Q, M, C, W = dims
    s = lax.axis_index("section")
    t = lax.axis_index("tensor")
    D = C * T
    heads = C // HEAD_DIM
    per = S * T // T // (S // 2) * T
    lane = lax.broadcasted_iota(jnp.int32, (M, LANES), 1)

    def dev(sec, ten):
        return {"section": sec, "tensor": ten}

    def weight_copies():
        cps = [
            pltpu.make_async_copy(wq_hbm, wcat.at[:, pl.ds(0, C)], w_sem.at[0]),
            pltpu.make_async_copy(wk_hbm, wcat.at[:, pl.ds(C, C)], w_sem.at[1]),
            pltpu.make_async_copy(wv_hbm, wcat.at[:, pl.ds(2 * C, C)], w_sem.at[2]),
            pltpu.make_async_copy(
                down_hbm,
                wcat.at[pl.ds(pl.multiple_of(t * C, C), C), pl.ds(3 * C, LANES)],
                w_sem.at[3],
            ),
        ]
        for b in range(T):
            cps.append(
                pltpu.make_async_copy(wo_hbm.at[:, pl.ds(b * C, C)], wout.at[b], w_sem.at[4 + b])
            )
        return cps

    for cp in weight_copies():
        cp.start()

    barrier = pltpu.get_barrier_semaphore()

    def greet(i, c):
        sec = i // T
        ten = i % T

        @pl.when(jnp.logical_not(jnp.logical_and(sec == s, ten == t)))
        def _():
            pl.semaphore_signal(barrier, inc=1, device_id=dev(sec, ten), device_id_type=MESH)

        return c

    lax.fori_loop(0, S * T, greet, 0)
    pl.semaphore_wait(barrier, S * T - 1)

    home = s // 2
    slot = (s % 2) * T + t

    def entry_copy(q):
        return pltpu.make_async_remote_copy(
            src_ref=xin_ref.at[q],
            dst_ref=ebuf.at[slot],
            send_sem=e_send.at[q],
            recv_sem=e_recv.at[slot],
            device_id=dev(q, home),
            device_id_type=MESH,
        )

    def entry_start(q, c):
        mine = jnp.logical_and(q == s, t == home)

        @pl.when(jnp.logical_not(mine))
        def _():
            entry_copy(q).start()

        @pl.when(mine)
        def _():
            ebuf[slot] = xin_ref[q]

        return c

    lax.fori_loop(0, S, entry_start, 0)

    def down_copy(k):
        return pltpu.make_async_remote_copy(
            src_ref=down_hbm,
            dst_ref=wcat.at[pl.ds(pl.multiple_of(t * C, C), C), pl.ds(3 * C, LANES)],
            send_sem=d_send.at[k - 1],
            recv_sem=d_recv.at[k - 1],
            device_id=dev(s, lax.rem(t + k, T)),
            device_id_type=MESH,
        )

    for k in (2, 1, 3):
        down_copy(k).start()

    upcat[...] = jnp.zeros_like(upcat)
    upcat[0 : upcat.shape[0] // 2, 0:C] = up_ref[0]
    upcat[upcat.shape[0] // 2 :, C:] = up_ref[1]

    def entry_wait(i, c):
        src_s = 2 * t + i // T
        src_t = i % T

        @pl.when(jnp.logical_not(jnp.logical_and(src_s == s, src_t == t)))
        def _():
            pltpu.make_async_remote_copy(
                src_ref=xin_ref.at[0],
                dst_ref=ebuf.at[i],
                send_sem=e_send.at[0],
                recv_sem=e_recv.at[i],
                device_id=dev(s, t),
                device_id_type=MESH,
            ).wait_recv()

        return c

    pieces = 2 * T
    lax.fori_loop(0, pieces, entry_wait, 0)
    blocks = [jnp.zeros((M, LANES), F32) for _ in range(C // LANES)]
    for i in range(pieces):
        b, o = divmod(i * W, LANES)
        val = ebuf[i].astype(F32)
        val = jnp.where(lane < W, val, 0.0)
        if o:
            val = pltpu.roll(val, o, 1)
        if o + W <= LANES:
            blocks[b] = blocks[b] + val
        else:
            blocks[b] = blocks[b] + jnp.where(lane >= o, val, 0.0)
            blocks[b + 1] = blocks[b + 1] + jnp.where(lane < o + W - LANES, val, 0.0)
    entered = jnp.concatenate(blocks, axis=1).astype(BF16)

    def entry_spread(k):
        return pltpu.make_async_remote_copy(
            src_ref=ag_out.at[Q],
            dst_ref=xbuf.at[s, t],
            send_sem=ea_send.at[k],
            recv_sem=x_recv.at[s, t],
            device_id=dev(0, lax.rem(t + k, T)),
            device_id_type=MESH,
        )

    ag_out[Q] = entered
    for k in (2, 1, 3):
        entry_spread(k).start()

    @pl.when(s > 0)
    def _():
        entry_spread(0).start()

    @pl.when(s == 0)
    def _():
        xbuf[0, t] = entered

    for cp in weight_copies():
        cp.wait()
    for k in (1, 3, 2):
        down_copy(k).wait_recv()

    row = lax.broadcasted_iota(jnp.int32, (M, M), 0)
    col = lax.broadcasted_iota(jnp.int32, (M, M), 1)
    causal = row >= col

    def rs_copy(q, k):
        other = lax.rem(t + k, T)
        return pltpu.make_async_remote_copy(
            src_ref=rs_out.at[q, k],
            dst_ref=rs_in.at[q, k],
            send_sem=rs_send.at[q, k],
            recv_sem=rs_recv.at[q, k],
            device_id=dev(s, other),
            device_id_type=MESH,
        )

    def ag_copy(q, k):
        return pltpu.make_async_remote_copy(
            src_ref=ag_out.at[q],
            dst_ref=xbuf.at[q, t],
            send_sem=ag_send.at[q, k],
            recv_sem=x_recv.at[q, t],
            device_id=dev(s + 1, lax.rem(t + k, T)),
            device_id_type=MESH,
        )

    def exit_copy(q, i):
        return pltpu.make_async_remote_copy(
            src_ref=xout.at[q, i],
            dst_ref=out_ref.at[q],
            send_sem=o_send.at[q, i],
            recv_sem=o_recv.at[q],
            device_id=dev(2 * t + i // T, i % T),
            device_id_type=MESH,
        )

    def phase_a(q):
        ss = jnp.zeros((M, LANES), F32)
        for k in (0, 1, 3, 2):
            p = lax.rem(t + k, T)

            def arrive():
                pltpu.make_async_remote_copy(
                    src_ref=ag_out.at[0],
                    dst_ref=xbuf.at[q, p],
                    send_sem=ag_send.at[0, 0],
                    recv_sem=x_recv.at[q, p],
                    device_id=dev(s, t),
                    device_id_type=MESH,
                ).wait_recv()

            if k == 0:
                pl.when(jnp.logical_not(jnp.logical_and(s == 0, q == 0)))(arrive)
            else:
                arrive()
            xf = xbuf[q, p].astype(F32)
            sq = xf * xf
            for b in range(C // LANES):
                ss = ss + sq[:, b * LANES : (b + 1) * LANES]
            xg = (xf * gain_ref[p]).astype(BF16)
            prod = jnp.dot(
                xg, wcat[pl.ds(pl.multiple_of(p * C, C), C), :], preferred_element_type=F32
            )
            if k == 0:
                acc[...] = prod
            else:
                acc[...] += prod
        return ss

    def phase_b(q, ss):
        r = lax.rsqrt(jnp.sum(ss, axis=1, keepdims=True) * (1.0 / D) + 1e-05)
        codes = (acc[:, 3 * C :] * r * mask_ref[q]).astype(BF16)
        low = jnp.dot(codes, upcat[...], preferred_element_type=F32)
        mixed = []
        for h in range(heads):
            a, b = h * HEAD_DIM, (h + 1) * HEAD_DIM
            qh = (acc[:, a:b] * r + low[:, a:b]).astype(BF16)
            kh = (acc[:, C + a : C + b] * r).astype(BF16)
            vh = (acc[:, 2 * C + a : 2 * C + b] * r + low[:, C + a : C + b]).astype(BF16)
            sc = lax.dot_general(
                qh, kh, (((1,), (1,)), ((), ())), preferred_element_type=F32
            ) * (HEAD_DIM ** (-0.5))
            sc = jnp.where(causal, sc, -jnp.inf)
            top = jnp.max(sc, axis=1, keepdims=True)
            wts = jnp.exp(sc - top)
            prob = (wts / jnp.sum(wts, axis=1, keepdims=True)).astype(BF16)
            mixed.append(jnp.dot(prob, vh, preferred_element_type=F32).astype(BF16))
        mix = jnp.concatenate(mixed, axis=1)
        for k in (2, 1, 3, 0):
            other = lax.rem(t + k, T)
            part = jnp.dot(mix, wout[other], preferred_element_type=F32).astype(BF16)
            rs_out[q, k] = part
            if k:
                rs_copy(q, k).start()

    def phase_c(q):
        total = xbuf[q, t].astype(F32) + rs_out[q, 0].astype(F32)
        for k in (1, 3, 2):
            rs_copy(q, k).wait_recv()
        for k in (1, 3, 2):
            total = total + rs_in[q, k].astype(F32)

        @pl.when(s < S - 1)
        def _():
            ag_out[q] = total.astype(BF16)
            for k in (2, 1, 3, 0):
                ag_copy(q, k).start()

        @pl.when(s == S - 1)
        def _():
            ag_out[q] = total.astype(BF16)
            for i in range(pieces):
                b, o = divmod(i * W, LANES)
                val = total[:, b * LANES : (b + 1) * LANES]
                if o + W > LANES:
                    nxt = total[:, (b + 1) * LANES : (b + 2) * LANES]
                    val = jnp.where(lane >= o, val, nxt)
                if o:
                    val = pltpu.roll(val, LANES - o, 1)
                xout[q, i] = val.astype(BF16)

            for i in range(pieces - 1):
                exit_copy(q, i).start()

            @pl.when(t < T - 1)
            def _():
                exit_copy(q, pieces - 1).start()

            @pl.when(t == T - 1)
            def _():
                out_ref[q] = xout[q, pieces - 1]

    def step(q, c):
        ss = phase_a(q)
        phase_b(q, ss)
        phase_c(q)
        return c

    lax.fori_loop(0, Q, step, 0)

    last = jnp.logical_and(s == S - 1, t == T - 1)

    def finish(q, c):
        @pl.when(jnp.logical_not(last))
        def _():
            pltpu.make_async_remote_copy(
                src_ref=xout.at[q, 0],
                dst_ref=out_ref.at[q],
                send_sem=o_send.at[q, 0],
                recv_sem=o_recv.at[q],
                device_id=dev(s, t),
                device_id_type=MESH,
            ).wait_recv()

        for k in (1, 2, 3):
            rs_copy(q, k).wait_send()

        @pl.when(s < S - 1)
        def _():
            for k in range(T):
                ag_copy(q, k).wait_send()

        @pl.when(s == S - 1)
        def _():
            for i in range(pieces - 1):
                exit_copy(q, i).wait_send()

            @pl.when(t < T - 1)
            def _():
                exit_copy(q, pieces - 1).wait_send()

        @pl.when(jnp.logical_not(jnp.logical_and(q == s, t == home)))
        def _():
            entry_copy(q).wait_send()

        return c

    lax.fori_loop(0, Q, finish, 0)
    for k in (1, 2, 3):
        down_copy(k).wait_send()
        entry_spread(k).wait_send()

    @pl.when(s > 0)
    def _():
        entry_spread(0).wait_send()


def shards(
    inputs,
    sequence_jobs,
    entry_sequence,
    layer_norm_gain,
    frozen_query_matrix,
    frozen_key_matrix,
    frozen_value_matrix,
    frozen_output_matrix,
    adapter_down_maps,
    adapter_up_maps,
):
    S = lax.axis_size("section")
    T = lax.axis_size("tensor")
    batches, groups, M, W = inputs.shape
    Q = batches * groups
    C = frozen_query_matrix.shape[2]
    D = C * T
    ranks = adapter_down_maps.shape[2]
    ordered = jnp.take(inputs, entry_sequence, axis=0).reshape(Q, M, W)
    xin = jnp.pad(ordered, ((0, 0), (0, 0), (0, LANES - W)))
    jobs = jnp.take(sequence_jobs, entry_sequence, axis=0).reshape(Q)
    column_job = jnp.arange(ranks, dtype=jnp.int32) // ADAPTER_RANK % ADAPTER_JOBS
    mask = jnp.where(column_job[None, :] == jobs[:, None], 2.0, 0.0).astype(F32).reshape(Q, 1, ranks)
    gain = layer_norm_gain.reshape(T, 1, C)

    vm = pl.BlockSpec(memory_space=pltpu.VMEM)
    hb = pl.BlockSpec(memory_space=pl.ANY)
    dma = pltpu.SemaphoreType.DMA
    out = pl.pallas_call(
        functools.partial(relay_kernel, (S, T, Q, M, C, W)),
        out_shape=jax.ShapeDtypeStruct((Q, M, LANES), BF16),
        in_specs=[vm, vm, vm, vm, hb, hb, hb, hb, hb],
        out_specs=vm,
        scratch_shapes=[
            pltpu.VMEM((D, 3 * C + ranks), BF16),
            pltpu.VMEM((T, C, C), BF16),
            pltpu.VMEM((ranks, 2 * C), BF16),
            pltpu.VMEM((Q, T, M, C), BF16),
            pltpu.VMEM((M, 3 * C + ranks), F32),
            pltpu.VMEM((Q, T, M, C), BF16),
            pltpu.VMEM((Q, T, M, C), BF16),
            pltpu.VMEM((Q + 1, M, C), BF16),
            pltpu.VMEM((2 * T, M, LANES), BF16),
            pltpu.VMEM((Q, 2 * T, M, LANES), BF16),
            dma((4 + T,)),
            dma((3,)),
            dma((3,)),
            dma((S,)),
            dma((2 * T,)),
            dma((T,)),
            dma((Q, T)),
            dma((Q, T)),
            dma((Q, T)),
            dma((Q, T)),
            dma((Q, 2 * T)),
            dma((Q,)),
        ],
        compiler_params=pltpu.CompilerParams(
            collective_id=0, has_side_effects=True, vmem_limit_bytes=56 * 1024 * 1024
        ),
        name="relay",
    )(
        xin,
        mask,
        gain,
        adapter_up_maps[0],
        adapter_down_maps[0],
        frozen_query_matrix[0],
        frozen_key_matrix[0],
        frozen_value_matrix[0],
        frozen_output_matrix[0],
    )
    return out[:, :, :W].reshape(batches, groups, M, W)


def solution(mesh):
    in_specs = (
        P("dp", None, None, ("section", "tensor")),
        P("dp", None, None),
        P("dp"),
        P("section", None),
        P("section", None, "tensor"),
        P("section", None, "tensor"),
        P("section", None, "tensor"),
        P("section", "tensor", None),
        P("section", "tensor", None),
        P("section", None, None, "tensor"),
    )
    out_specs = P("dp", None, None, ("section", "tensor"))
    return jax.shard_map(shards, mesh=mesh, in_specs=in_specs, out_specs=out_specs, check_vma=False)
```

```python
import functools

import jax
import jax.numpy as jnp
from jax import lax
from jax.experimental import pallas as pl
from jax.experimental.pallas import tpu as pltpu
from jax.sharding import PartitionSpec as P

HEAD_DIM = 128
ADAPTER_RANK = 16
ADAPTER_JOBS = 4
LANES = 128
UNITS_PER_SEQUENCE = 2
MESH = pl.DeviceIdType.MESH
F32 = jnp.float32
BF16 = jnp.bfloat16


def relay_kernel(
    dims,
    entry_ref,
    jobs_ref,
    xin_ref,
    gain_ref,
    up_ref,
    down_hbm,
    wq_hbm,
    wk_hbm,
    wv_hbm,
    wo_hbm,
    out_ref,
    wcat,
    wout,
    upcat,
    kbuf,
    vbuf,
    xbuf,
    acc,
    rs_out,
    rs_in,
    ag_out,
    estage,
    ebuf,
    xout,
    w_sem,
    d_send,
    d_recv,
    e_send,
    e_recv,
    ea_send,
    x_recv,
    ag_send,
    rs_send,
    rs_recv,
    o_send,
    o_recv,
):
    S, T, Q, L, H, C, W = dims
    M = L // H
    U = Q * H
    groups = xin_ref.shape[1]
    s = lax.axis_index("section")
    t = lax.axis_index("tensor")
    D = C * T
    heads = C // HEAD_DIM
    lane = lax.broadcasted_iota(jnp.int32, (M, LANES), 1)
    long_lane = lax.broadcasted_iota(jnp.int32, (L, LANES), 1)

    def dev(sec, ten):
        return {"section": sec, "tensor": ten}

    def weight_copies():
        cps = [
            pltpu.make_async_copy(wq_hbm, wcat.at[:, pl.ds(0, C)], w_sem.at[0]),
            pltpu.make_async_copy(wk_hbm, wcat.at[:, pl.ds(C, C)], w_sem.at[1]),
            pltpu.make_async_copy(wv_hbm, wcat.at[:, pl.ds(2 * C, C)], w_sem.at[2]),
            pltpu.make_async_copy(
                down_hbm,
                wcat.at[pl.ds(pl.multiple_of(t * C, C), C), pl.ds(3 * C, LANES)],
                w_sem.at[3],
            ),
        ]
        for b in range(T):
            cps.append(
                pltpu.make_async_copy(wo_hbm.at[:, pl.ds(b * C, C)], wout.at[b], w_sem.at[4 + b])
            )
        return cps

    for cp in weight_copies():
        cp.start()

    barrier = pltpu.get_barrier_semaphore()

    def greet(i, c):
        sec = i // T
        ten = i % T

        @pl.when(jnp.logical_not(jnp.logical_and(sec == s, ten == t)))
        def _():
            pl.semaphore_signal(barrier, inc=1, device_id=dev(sec, ten), device_id_type=MESH)

        return c

    lax.fori_loop(0, S * T, greet, 0)

    estage[...] = jnp.zeros_like(estage)
    for q in range(Q):
        estage[q, :, 0:W] = xin_ref[entry_ref[q // groups], q % groups]
    kbuf[...] = jnp.zeros_like(kbuf)
    vbuf[...] = jnp.zeros_like(vbuf)
    upcat[...] = jnp.zeros_like(upcat)
    upcat[0 : upcat.shape[0] // 2, 0:C] = up_ref[0]
    upcat[upcat.shape[0] // 2 :, C:] = up_ref[1]
    pl.semaphore_wait(barrier, S * T - 1)

    home = s // 2
    slot = (s % 2) * T + t

    def entry_copy(q):
        return pltpu.make_async_remote_copy(
            src_ref=estage.at[q],
            dst_ref=ebuf.at[slot],
            send_sem=e_send.at[q],
            recv_sem=e_recv.at[slot],
            device_id=dev(q, home),
            device_id_type=MESH,
        )

    def entry_start(q, c):
        mine = jnp.logical_and(q == s, t == home)

        @pl.when(jnp.logical_not(mine))
        def _():
            entry_copy(q).start()

        @pl.when(mine)
        def _():
            ebuf[slot] = estage[q]

        return c

    lax.fori_loop(0, S, entry_start, 0)

    def down_copy(k):
        return pltpu.make_async_remote_copy(
            src_ref=down_hbm,
            dst_ref=wcat.at[pl.ds(pl.multiple_of(t * C, C), C), pl.ds(3 * C, LANES)],
            send_sem=d_send.at[k - 1],
            recv_sem=d_recv.at[k - 1],
            device_id=dev(s, lax.rem(t + k, T)),
            device_id_type=MESH,
        )

    @pl.when(s == 0)
    def _():
        for k in (2, 1, 3):
            down_copy(k).start()

    def entry_wait(i, c):
        src_s = 2 * t + i // T
        src_t = i % T

        @pl.when(jnp.logical_not(jnp.logical_and(src_s == s, src_t == t)))
        def _():
            pltpu.make_async_remote_copy(
                src_ref=estage.at[0],
                dst_ref=ebuf.at[i],
                send_sem=e_send.at[0],
                recv_sem=e_recv.at[i],
                device_id=dev(s, t),
                device_id_type=MESH,
            ).wait_recv()

        return c

    pieces = 2 * T
    lax.fori_loop(0, pieces, entry_wait, 0)
    blocks = [jnp.zeros((L, LANES), F32) for _ in range(C // LANES)]
    for i in range(pieces):
        b, o = divmod(i * W, LANES)
        val = ebuf[i].astype(F32)
        val = jnp.where(long_lane < W, val, 0.0)
        if o:
            val = pltpu.roll(val, o, 1)
        if o + W <= LANES:
            blocks[b] = blocks[b] + val
        else:
            blocks[b] = blocks[b] + jnp.where(long_lane >= o, val, 0.0)
            blocks[b + 1] = blocks[b + 1] + jnp.where(long_lane < o + W - LANES, val, 0.0)
    entered = jnp.concatenate(blocks, axis=1).astype(BF16)

    def entry_spread(h, k):
        return pltpu.make_async_remote_copy(
            src_ref=ag_out.at[U + h],
            dst_ref=xbuf.at[H * s + h, t],
            send_sem=ea_send.at[h, k],
            recv_sem=x_recv.at[H * s + h, t],
            device_id=dev(0, lax.rem(t + k, T)),
            device_id_type=MESH,
        )

    for h in range(H):
        ag_out[U + h] = entered[h * M : (h + 1) * M]
        for k in (2, 1, 3):
            entry_spread(h, k).start()

        @pl.when(s > 0)
        def _():
            entry_spread(h, 0).start()

        @pl.when(s == 0)
        def _():
            xbuf[h, t] = entered[h * M : (h + 1) * M]

    @pl.when(s > 0)
    def _():
        for k in (2, 1, 3):
            down_copy(k).start()

    for cp in weight_copies():
        cp.wait()
    for k in (1, 3, 2):
        down_copy(k).wait_recv()

    row = lax.broadcasted_iota(jnp.int32, (M, L), 0)
    col = lax.broadcasted_iota(jnp.int32, (M, L), 1)
    owner = lax.broadcasted_iota(jnp.int32, (1, LANES), 1) // ADAPTER_RANK % ADAPTER_JOBS

    def rs_copy(q, k):
        other = lax.rem(t + k, T)
        return pltpu.make_async_remote_copy(
            src_ref=rs_out.at[q, k],
            dst_ref=rs_in.at[q, k],
            send_sem=rs_send.at[q, k],
            recv_sem=rs_recv.at[q, k],
            device_id=dev(s, other),
            device_id_type=MESH,
        )

    def ag_copy(q, k):
        return pltpu.make_async_remote_copy(
            src_ref=ag_out.at[q],
            dst_ref=xbuf.at[q, t],
            send_sem=ag_send.at[q, k],
            recv_sem=x_recv.at[q, t],
            device_id=dev(s + 1, lax.rem(t + k, T)),
            device_id_type=MESH,
        )

    def exit_copy(q, i):
        return pltpu.make_async_remote_copy(
            src_ref=xout.at[q, i],
            dst_ref=out_ref.at[q],
            send_sem=o_send.at[q, i],
            recv_sem=o_recv.at[q],
            device_id=dev(2 * t + i // T, i % T),
            device_id_type=MESH,
        )

    def phase_a(q):
        ss = jnp.zeros((M, LANES), F32)
        for k in (0, 1, 3, 2):
            p = lax.rem(t + k, T)

            def arrive():
                pltpu.make_async_remote_copy(
                    src_ref=ag_out.at[0],
                    dst_ref=xbuf.at[q, p],
                    send_sem=ag_send.at[0, 0],
                    recv_sem=x_recv.at[q, p],
                    device_id=dev(s, t),
                    device_id_type=MESH,
                ).wait_recv()

            if k == 0:
                pl.when(jnp.logical_not(jnp.logical_and(s == 0, q < H)))(arrive)
            else:
                arrive()
            xf = xbuf[q, p].astype(F32)
            sq = xf * xf
            for b in range(C // LANES):
                ss = ss + sq[:, b * LANES : (b + 1) * LANES]
            xg = (xf * gain_ref[p]).astype(BF16)
            prod = jnp.dot(
                xg, wcat[pl.ds(pl.multiple_of(p * C, C), C), :], preferred_element_type=F32
            )
            if k == 0:
                acc[...] = prod
            else:
                acc[...] += prod
        return ss

    def phase_b(q, ss):
        r = lax.rsqrt(jnp.sum(ss, axis=1, keepdims=True) * (1.0 / D) + 1e-05)
        seq = q // H
        part = q % H
        job = jobs_ref[seq % groups, entry_ref[seq // groups]]
        codes = jnp.where(owner == job, acc[:, 3 * C :] * (r * 2.0), 0.0).astype(BF16)
        low = jnp.dot(codes, upcat[...], preferred_element_type=F32)
        here = pl.ds(pl.multiple_of(part * M, M), M)
        kbuf[here, :] = (acc[:, C : 2 * C] * r).astype(BF16)
        vbuf[here, :] = (acc[:, 2 * C : 3 * C] * r + low[:, C:]).astype(BF16)
        causal = row + part * M >= col
        mixed = []
        for h in range(heads):
            a, b = h * HEAD_DIM, (h + 1) * HEAD_DIM
            qh = (acc[:, a:b] * r + low[:, a:b]).astype(BF16)
            kh = kbuf[:, a:b]
            vh = vbuf[:, a:b]
            sc = lax.dot_general(
                qh, kh, (((1,), (1,)), ((), ())), preferred_element_type=F32
            ) * (HEAD_DIM ** (-0.5))
            sc = jnp.where(causal, sc, -jnp.inf)
            top = jnp.max(sc, axis=1, keepdims=True)
            wts = jnp.exp(sc - top)
            prob = (wts / jnp.sum(wts, axis=1, keepdims=True)).astype(BF16)
            mixed.append(jnp.dot(prob, vh, preferred_element_type=F32).astype(BF16))
        mix = jnp.concatenate(mixed, axis=1)
        for k in (2, 1, 3, 0):
            other = lax.rem(t + k, T)
            rs_out[q, k] = jnp.dot(mix, wout[other], preferred_element_type=F32).astype(BF16)
            if k:
                rs_copy(q, k).start()

    def phase_c(q):
        total = xbuf[q, t].astype(F32) + rs_out[q, 0].astype(F32)
        for k in (1, 3, 2):
            rs_copy(q, k).wait_recv()
        for k in (1, 3, 2):
            total = total + rs_in[q, k].astype(F32)

        @pl.when(s < S - 1)
        def _():
            ag_out[q] = total.astype(BF16)
            for k in (2, 1, 3, 0):
                ag_copy(q, k).start()

        @pl.when(s == S - 1)
        def _():
            ag_out[q] = total.astype(BF16)
            for i in range(pieces):
                b, o = divmod(i * W, LANES)
                val = total[:, b * LANES : (b + 1) * LANES]
                if o + W > LANES:
                    nxt = total[:, (b + 1) * LANES : (b + 2) * LANES]
                    val = jnp.where(lane >= o, val, nxt)
                if o:
                    val = pltpu.roll(val, LANES - o, 1)
                xout[q, i] = val.astype(BF16)

            for i in range(pieces - 1):
                exit_copy(q, i).start()

            @pl.when(t < T - 1)
            def _():
                exit_copy(q, pieces - 1).start()

            @pl.when(t == T - 1)
            def _():
                out_ref[q] = xout[q, pieces - 1]

    def step(q, c):
        @pl.when(q < U)
        def _():
            ss = phase_a(q)
            phase_b(q, ss)

        @pl.when(q > 0)
        def _():
            phase_c(q - 1)

        return c

    lax.fori_loop(0, U + 1, step, 0)

    last = jnp.logical_and(s == S - 1, t == T - 1)

    def finish(q, c):
        @pl.when(jnp.logical_not(last))
        def _():
            pltpu.make_async_remote_copy(
                src_ref=xout.at[q, 0],
                dst_ref=out_ref.at[q],
                send_sem=o_send.at[q, 0],
                recv_sem=o_recv.at[q],
                device_id=dev(s, t),
                device_id_type=MESH,
            ).wait_recv()

        for k in (1, 2, 3):
            rs_copy(q, k).wait_send()

        @pl.when(s < S - 1)
        def _():
            for k in range(T):
                ag_copy(q, k).wait_send()

        @pl.when(s == S - 1)
        def _():
            for i in range(pieces - 1):
                exit_copy(q, i).wait_send()

            @pl.when(t < T - 1)
            def _():
                exit_copy(q, pieces - 1).wait_send()

        return c

    lax.fori_loop(0, U, finish, 0)
    for q in range(S):

        @pl.when(jnp.logical_not(jnp.logical_and(s == q, t == home)))
        def _():
            entry_copy(q).wait_send()

    for k in (1, 2, 3):
        down_copy(k).wait_send()
        for h in range(H):
            entry_spread(h, k).wait_send()

    @pl.when(s > 0)
    def _():
        for h in range(H):
            entry_spread(h, 0).wait_send()


def shards(
    inputs,
    sequence_jobs,
    entry_sequence,
    layer_norm_gain,
    frozen_query_matrix,
    frozen_key_matrix,
    frozen_value_matrix,
    frozen_output_matrix,
    adapter_down_maps,
    adapter_up_maps,
):
    S = lax.axis_size("section")
    T = lax.axis_size("tensor")
    batches, groups, L, W = inputs.shape
    Q = batches * groups
    H = UNITS_PER_SEQUENCE
    U, M = Q * H, L // H
    C = frozen_query_matrix.shape[2]
    D = C * T
    ranks = adapter_down_maps.shape[2]
    jobs = jnp.transpose(sequence_jobs, (1, 2, 0)).reshape(groups, batches)
    gain = layer_norm_gain.reshape(T, 1, C)

    vm = pl.BlockSpec(memory_space=pltpu.VMEM)
    hb = pl.BlockSpec(memory_space=pl.ANY)
    sm = pl.BlockSpec(memory_space=pltpu.SMEM)
    dma = pltpu.SemaphoreType.DMA
    out = pl.pallas_call(
        functools.partial(relay_kernel, (S, T, Q, L, H, C, W)),
        out_shape=jax.ShapeDtypeStruct((U, M, LANES), BF16),
        in_specs=[sm, sm, vm, vm, vm, hb, hb, hb, hb, hb],
        out_specs=vm,
        scratch_shapes=[
            pltpu.VMEM((D, 3 * C + ranks), BF16),
            pltpu.VMEM((T, C, C), BF16),
            pltpu.VMEM((ranks, 2 * C), BF16),
            pltpu.VMEM((L, C), BF16),
            pltpu.VMEM((L, C), BF16),
            pltpu.VMEM((U, T, M, C), BF16),
            pltpu.VMEM((M, 3 * C + ranks), F32),
            pltpu.VMEM((U, T, M, C), BF16),
            pltpu.VMEM((U, T, M, C), BF16),
            pltpu.VMEM((U + H, M, C), BF16),
            pltpu.VMEM((Q, L, LANES), BF16),
            pltpu.VMEM((2 * T, L, LANES), BF16),
            pltpu.VMEM((U, 2 * T, M, LANES), BF16),
            dma((4 + T,)),
            dma((3,)),
            dma((3,)),
            dma((S,)),
            dma((2 * T,)),
            dma((H, T)),
            dma((U, T)),
            dma((U, T)),
            dma((U, T)),
            dma((U, T)),
            dma((U, 2 * T)),
            dma((U,)),
        ],
        compiler_params=pltpu.CompilerParams(
            collective_id=0, has_side_effects=True, vmem_limit_bytes=56 * 1024 * 1024
        ),
        name="relay",
    )(
        entry_sequence,
        jobs,
        inputs,
        gain,
        adapter_up_maps[0],
        adapter_down_maps[0],
        frozen_query_matrix[0],
        frozen_key_matrix[0],
        frozen_value_matrix[0],
        frozen_output_matrix[0],
    )
    return out[:, :, :W].reshape(batches, groups, L, W)


def solution(mesh):
    in_specs = (
        P("dp", None, None, ("section", "tensor")),
        P("dp", None, None),
        P("dp"),
        P("section", None),
        P("section", None, "tensor"),
        P("section", None, "tensor"),
        P("section", None, "tensor"),
        P("section", "tensor", None),
        P("section", "tensor", None),
        P("section", None, None, "tensor"),
    )
    out_specs = P("dp", None, None, ("section", "tensor"))
    return jax.shard_map(shards, mesh=mesh, in_specs=in_specs, out_specs=out_specs, check_vma=False)
```

```python
import functools

import jax
import jax.numpy as jnp
from jax import lax
from jax.experimental import pallas as pl
from jax.experimental.pallas import tpu as pltpu
from jax.sharding import PartitionSpec as P

HEAD_DIM = 128
ADAPTER_RANK = 16
ADAPTER_JOBS = 4
LANES = 128
UNITS_PER_SEQUENCE = 2
MESH = pl.DeviceIdType.MESH
F32 = jnp.float32
BF16 = jnp.bfloat16


def relay_kernel(
    dims,
    entry_ref,
    jobs_ref,
    xin_ref,
    gain_ref,
    up_ref,
    down_hbm,
    wq_hbm,
    wk_hbm,
    wv_hbm,
    wo_hbm,
    out_ref,
    wcat,
    wout,
    upcat,
    kbuf,
    vbuf,
    xbuf,
    acc,
    rs_out,
    rs_in,
    ag_out,
    estage,
    ebuf,
    xout,
    w_sem,
    d_send,
    d_recv,
    e_send,
    e_recv,
    ea_send,
    x_recv,
    ag_send,
    rs_send,
    rs_recv,
    o_send,
    o_recv,
):
    S, T, Q, L, H, C, W = dims
    M = L // H
    U = Q * H
    groups = xin_ref.shape[1]
    s = lax.axis_index("section")
    t = lax.axis_index("tensor")
    D = C * T
    heads = C // HEAD_DIM
    lane = lax.broadcasted_iota(jnp.int32, (M, LANES), 1)
    long_lane = lax.broadcasted_iota(jnp.int32, (L, LANES), 1)

    def dev(sec, ten):
        return {"section": sec, "tensor": ten}

    def weight_copies():
        cps = [
            pltpu.make_async_copy(wq_hbm, wcat.at[:, pl.ds(LANES, C)], w_sem.at[0]),
            pltpu.make_async_copy(wk_hbm, wcat.at[:, pl.ds(LANES + C, C)], w_sem.at[1]),
            pltpu.make_async_copy(wv_hbm, wcat.at[:, pl.ds(LANES + 2 * C, C)], w_sem.at[2]),
            pltpu.make_async_copy(
                down_hbm,
                wcat.at[pl.ds(pl.multiple_of(t * C, C), C), pl.ds(0, LANES)],
                w_sem.at[3],
            ),
        ]
        for b in range(T):
            cps.append(
                pltpu.make_async_copy(wo_hbm.at[:, pl.ds(b * C, C)], wout.at[b], w_sem.at[4 + b])
            )
        return cps

    for cp in weight_copies():
        cp.start()

    barrier = pltpu.get_barrier_semaphore()

    def greet(i, c):
        sec = i // T
        ten = i % T

        @pl.when(jnp.logical_not(jnp.logical_and(sec == s, ten == t)))
        def _():
            pl.semaphore_signal(barrier, inc=1, device_id=dev(sec, ten), device_id_type=MESH)

        return c

    lax.fori_loop(0, S * T, greet, 0)

    estage[...] = jnp.zeros_like(estage)
    for q in range(Q):
        estage[q, :, 0:W] = xin_ref[entry_ref[q // groups], q % groups]
    kbuf[...] = jnp.zeros_like(kbuf)
    vbuf[...] = jnp.zeros_like(vbuf)
    upcat[...] = jnp.zeros_like(upcat)
    upcat[0 : upcat.shape[0] // 2, 0:C] = up_ref[0]
    upcat[upcat.shape[0] // 2 :, C:] = up_ref[1]
    pl.semaphore_wait(barrier, S * T - 1)

    home = s // 2
    slot = (s % 2) * T + t

    def entry_copy(q):
        return pltpu.make_async_remote_copy(
            src_ref=estage.at[q],
            dst_ref=ebuf.at[slot],
            send_sem=e_send.at[q],
            recv_sem=e_recv.at[slot],
            device_id=dev(q, home),
            device_id_type=MESH,
        )

    def entry_start(q, c):
        mine = jnp.logical_and(q == s, t == home)

        @pl.when(jnp.logical_not(mine))
        def _():
            entry_copy(q).start()

        @pl.when(mine)
        def _():
            ebuf[slot] = estage[q]

        return c

    lax.fori_loop(0, S, entry_start, 0)

    def down_copy(k):
        return pltpu.make_async_remote_copy(
            src_ref=down_hbm,
            dst_ref=wcat.at[pl.ds(pl.multiple_of(t * C, C), C), pl.ds(0, LANES)],
            send_sem=d_send.at[k - 1],
            recv_sem=d_recv.at[k - 1],
            device_id=dev(s, lax.rem(t + k, T)),
            device_id_type=MESH,
        )

    @pl.when(s == 0)
    def _():
        for k in (2, 1, 3):
            down_copy(k).start()

    def entry_wait(i, c):
        src_s = 2 * t + i // T
        src_t = i % T

        @pl.when(jnp.logical_not(jnp.logical_and(src_s == s, src_t == t)))
        def _():
            pltpu.make_async_remote_copy(
                src_ref=estage.at[0],
                dst_ref=ebuf.at[i],
                send_sem=e_send.at[0],
                recv_sem=e_recv.at[i],
                device_id=dev(s, t),
                device_id_type=MESH,
            ).wait_recv()

        return c

    pieces = 2 * T
    lax.fori_loop(0, pieces, entry_wait, 0)
    blocks = [jnp.zeros((L, LANES), F32) for _ in range(C // LANES)]
    for i in range(pieces):
        b, o = divmod(i * W, LANES)
        val = ebuf[i].astype(F32)
        val = jnp.where(long_lane < W, val, 0.0)
        if o:
            val = pltpu.roll(val, o, 1)
        if o + W <= LANES:
            blocks[b] = blocks[b] + val
        else:
            blocks[b] = blocks[b] + jnp.where(long_lane >= o, val, 0.0)
            blocks[b + 1] = blocks[b + 1] + jnp.where(long_lane < o + W - LANES, val, 0.0)
    entered = jnp.concatenate(blocks, axis=1).astype(BF16)

    def entry_spread(h, k):
        return pltpu.make_async_remote_copy(
            src_ref=ag_out.at[U + h],
            dst_ref=xbuf.at[H * s + h, t],
            send_sem=ea_send.at[h, k],
            recv_sem=x_recv.at[H * s + h, t],
            device_id=dev(0, lax.rem(t + k, T)),
            device_id_type=MESH,
        )

    for h in range(H):
        ag_out[U + h] = entered[h * M : (h + 1) * M]
        for k in (2, 1, 3):
            entry_spread(h, k).start()

        @pl.when(s > 0)
        def _():
            entry_spread(h, 0).start()

        @pl.when(s == 0)
        def _():
            xbuf[h, t] = entered[h * M : (h + 1) * M]

    @pl.when(s > 0)
    def _():
        for k in (2, 1, 3):
            down_copy(k).start()

    for cp in weight_copies():
        cp.wait()
    for k in (1, 3, 2):
        down_copy(k).wait_recv()

    row = lax.broadcasted_iota(jnp.int32, (M, L), 0)
    col = lax.broadcasted_iota(jnp.int32, (M, L), 1)
    owner = lax.broadcasted_iota(jnp.int32, (1, LANES), 1) // ADAPTER_RANK % ADAPTER_JOBS

    def rs_copy(q, k):
        other = lax.rem(t + k, T)
        return pltpu.make_async_remote_copy(
            src_ref=rs_out.at[q, k],
            dst_ref=rs_in.at[q, k],
            send_sem=rs_send.at[q, k],
            recv_sem=rs_recv.at[q, k],
            device_id=dev(s, other),
            device_id_type=MESH,
        )

    def ag_copy(q, k):
        return pltpu.make_async_remote_copy(
            src_ref=ag_out.at[q],
            dst_ref=xbuf.at[q, t],
            send_sem=ag_send.at[q, k],
            recv_sem=x_recv.at[q, t],
            device_id=dev(s + 1, lax.rem(t + k, T)),
            device_id_type=MESH,
        )

    def exit_copy(q, i):
        return pltpu.make_async_remote_copy(
            src_ref=xout.at[q, i],
            dst_ref=out_ref.at[q],
            send_sem=o_send.at[q, i],
            recv_sem=o_recv.at[q],
            device_id=dev(2 * t + i // T, i % T),
            device_id_type=MESH,
        )

    def arrive(q, p):
        pltpu.make_async_remote_copy(
            src_ref=ag_out.at[0],
            dst_ref=xbuf.at[q, p],
            send_sem=ag_send.at[0, 0],
            recv_sem=x_recv.at[q, p],
            device_id=dev(s, t),
            device_id_type=MESH,
        ).wait_recv()

    def product(q, ks, ss):
        total = None
        for k in ks:
            p = lax.rem(t + k, T)
            xf = xbuf[q, p].astype(F32)
            sq = xf * xf
            for b in range(C // LANES):
                ss = ss + sq[:, b * LANES : (b + 1) * LANES]
            xg = (xf * gain_ref[p]).astype(BF16)
            prod = jnp.dot(
                xg, wcat[pl.ds(pl.multiple_of(p * C, C), C), :], preferred_element_type=F32
            )
            total = prod if total is None else total + prod
        return total, ss

    def phase_a(q):
        pl.when(jnp.logical_not(jnp.logical_and(s == 0, q < H)))(lambda: arrive(q, t))
        for k in (1, 3):
            arrive(q, lax.rem(t + k, T))
        acc[...], ss = product(q, (0, 1, 3), jnp.zeros((M, LANES), F32))
        arrive(q, lax.rem(t + 2, T))
        last, ss = product(q, (2,), ss)
        acc[...] += last
        return ss

    def phase_b(q, ss):
        r = lax.rsqrt(jnp.sum(ss, axis=1, keepdims=True) * (1.0 / D) + 1e-05)
        seq = q // H
        part = q % H
        job = jobs_ref[seq % groups, entry_ref[seq // groups]]
        codes = jnp.where(owner == job, acc[:, :LANES] * (r * 2.0), 0.0).astype(BF16)
        low = jnp.dot(codes, upcat[...], preferred_element_type=F32)
        here = pl.ds(pl.multiple_of(part * M, M), M)
        q0, k0, v0 = LANES, LANES + C, LANES + 2 * C
        kbuf[here, :] = (acc[:, k0:v0] * r).astype(BF16)
        vbuf[here, :] = (acc[:, v0 : v0 + C] * r + low[:, C:]).astype(BF16)
        causal = row + part * M >= col
        mixed = []
        for h in range(heads):
            a, b = h * HEAD_DIM, (h + 1) * HEAD_DIM
            qh = (acc[:, q0 + a : q0 + b] * r + low[:, a:b]).astype(BF16)
            sc = lax.dot_general(
                qh, kbuf[:, a:b], (((1,), (1,)), ((), ())), preferred_element_type=F32
            ) * (HEAD_DIM ** (-0.5))
            sc = jnp.where(causal, sc, -jnp.inf)
            wts = jnp.exp(sc - jnp.max(sc, axis=1, keepdims=True))
            mean = jnp.dot(wts.astype(BF16), vbuf[:, a:b], preferred_element_type=F32)
            mixed.append((mean / jnp.sum(wts, axis=1, keepdims=True)).astype(BF16))
        mix = jnp.concatenate(mixed, axis=1)
        for k in (2, 1, 3, 0):
            other = lax.rem(t + k, T)
            rs_out[q, k] = jnp.dot(mix, wout[other], preferred_element_type=F32).astype(BF16)
        for k in (2, 1, 3):
            rs_copy(q, k).start()

    def phase_c(q):
        total = xbuf[q, t].astype(F32) + rs_out[q, 0].astype(F32)
        for k in (1, 3, 2):
            rs_copy(q, k).wait_recv()
        for k in (1, 3, 2):
            total = total + rs_in[q, k].astype(F32)

        @pl.when(s < S - 1)
        def _():
            ag_out[q] = total.astype(BF16)
            for k in (2, 1, 3, 0):
                ag_copy(q, k).start()

        @pl.when(s == S - 1)
        def _():
            ag_out[q] = total.astype(BF16)
            for i in range(pieces):
                b, o = divmod(i * W, LANES)
                val = total[:, b * LANES : (b + 1) * LANES]
                if o + W > LANES:
                    nxt = total[:, (b + 1) * LANES : (b + 2) * LANES]
                    val = jnp.where(lane >= o, val, nxt)
                if o:
                    val = pltpu.roll(val, LANES - o, 1)
                xout[q, i] = val.astype(BF16)

            for i in range(pieces - 1):
                exit_copy(q, i).start()

            @pl.when(t < T - 1)
            def _():
                exit_copy(q, pieces - 1).start()

            @pl.when(t == T - 1)
            def _():
                out_ref[q] = xout[q, pieces - 1]

    def step(q, c):
        @pl.when(q < U)
        def _():
            ss = phase_a(q)
            phase_b(q, ss)

        @pl.when(q > 0)
        def _():
            phase_c(q - 1)

        return c

    lax.fori_loop(0, U + 1, step, 0)

    last = jnp.logical_and(s == S - 1, t == T - 1)

    def finish(q, c):
        @pl.when(jnp.logical_not(last))
        def _():
            pltpu.make_async_remote_copy(
                src_ref=xout.at[q, 0],
                dst_ref=out_ref.at[q],
                send_sem=o_send.at[q, 0],
                recv_sem=o_recv.at[q],
                device_id=dev(s, t),
                device_id_type=MESH,
            ).wait_recv()

        for k in (1, 2, 3):
            rs_copy(q, k).wait_send()

        @pl.when(s < S - 1)
        def _():
            for k in range(T):
                ag_copy(q, k).wait_send()

        @pl.when(s == S - 1)
        def _():
            for i in range(pieces - 1):
                exit_copy(q, i).wait_send()

            @pl.when(t < T - 1)
            def _():
                exit_copy(q, pieces - 1).wait_send()

        return c

    lax.fori_loop(0, U, finish, 0)
    for q in range(S):

        @pl.when(jnp.logical_not(jnp.logical_and(s == q, t == home)))
        def _():
            entry_copy(q).wait_send()

    for k in (1, 2, 3):
        down_copy(k).wait_send()
        for h in range(H):
            entry_spread(h, k).wait_send()

    @pl.when(s > 0)
    def _():
        for h in range(H):
            entry_spread(h, 0).wait_send()


def shards(
    inputs,
    sequence_jobs,
    entry_sequence,
    layer_norm_gain,
    frozen_query_matrix,
    frozen_key_matrix,
    frozen_value_matrix,
    frozen_output_matrix,
    adapter_down_maps,
    adapter_up_maps,
):
    S = lax.axis_size("section")
    T = lax.axis_size("tensor")
    batches, groups, L, W = inputs.shape
    Q = batches * groups
    H = UNITS_PER_SEQUENCE
    U, M = Q * H, L // H
    C = frozen_query_matrix.shape[2]
    D = C * T
    ranks = adapter_down_maps.shape[2]
    jobs = jnp.transpose(sequence_jobs, (1, 2, 0)).reshape(groups, batches)
    gain = layer_norm_gain.reshape(T, 1, C)

    vm = pl.BlockSpec(memory_space=pltpu.VMEM)
    hb = pl.BlockSpec(memory_space=pl.ANY)
    sm = pl.BlockSpec(memory_space=pltpu.SMEM)
    dma = pltpu.SemaphoreType.DMA
    out = pl.pallas_call(
        functools.partial(relay_kernel, (S, T, Q, L, H, C, W)),
        out_shape=jax.ShapeDtypeStruct((U, M, LANES), BF16),
        in_specs=[sm, sm, vm, vm, vm, hb, hb, hb, hb, hb],
        out_specs=vm,
        scratch_shapes=[
            pltpu.VMEM((D, 3 * C + ranks), BF16),
            pltpu.VMEM((T, C, C), BF16),
            pltpu.VMEM((ranks, 2 * C), BF16),
            pltpu.VMEM((L, C), BF16),
            pltpu.VMEM((L, C), BF16),
            pltpu.VMEM((U, T, M, C), BF16),
            pltpu.VMEM((M, 3 * C + ranks), F32),
            pltpu.VMEM((U, T, M, C), BF16),
            pltpu.VMEM((U, T, M, C), BF16),
            pltpu.VMEM((U + H, M, C), BF16),
            pltpu.VMEM((Q, L, LANES), BF16),
            pltpu.VMEM((2 * T, L, LANES), BF16),
            pltpu.VMEM((U, 2 * T, M, LANES), BF16),
            dma((4 + T,)),
            dma((3,)),
            dma((3,)),
            dma((S,)),
            dma((2 * T,)),
            dma((H, T)),
            dma((U, T)),
            dma((U, T)),
            dma((U, T)),
            dma((U, T)),
            dma((U, 2 * T)),
            dma((U,)),
        ],
        compiler_params=pltpu.CompilerParams(
            collective_id=0, has_side_effects=True, vmem_limit_bytes=56 * 1024 * 1024
        ),
        name="relay",
    )(
        entry_sequence,
        jobs,
        inputs,
        gain,
        adapter_up_maps[0],
        adapter_down_maps[0],
        frozen_query_matrix[0],
        frozen_key_matrix[0],
        frozen_value_matrix[0],
        frozen_output_matrix[0],
    )
    return out[:, :, :W].reshape(batches, groups, L, W)


def solution(mesh):
    in_specs = (
        P("dp", None, None, ("section", "tensor")),
        P("dp", None, None),
        P("dp"),
        P("section", None),
        P("section", None, "tensor"),
        P("section", None, "tensor"),
        P("section", None, "tensor"),
        P("section", "tensor", None),
        P("section", "tensor", None),
        P("section", None, None, "tensor"),
    )
    out_specs = P("dp", None, None, ("section", "tensor"))
    return jax.shard_map(shards, mesh=mesh, in_specs=in_specs, out_specs=out_specs, check_vma=False)
```

```python
import functools

import jax
import jax.numpy as jnp
from jax import lax
from jax.experimental import pallas as pl
from jax.experimental.pallas import tpu as pltpu
from jax.sharding import PartitionSpec as P

HEAD_DIM = 128
ADAPTER_RANK = 16
ADAPTER_JOBS = 4
LANES = 128
UNITS_PER_SEQUENCE = 2
MESH = pl.DeviceIdType.MESH
F32 = jnp.float32
BF16 = jnp.bfloat16


def relay_kernel(
    dims,
    entry_ref,
    jobs_ref,
    xin_ref,
    gain_ref,
    up_ref,
    down_hbm,
    wq_hbm,
    wk_hbm,
    wv_hbm,
    wo_hbm,
    out_ref,
    wcat,
    wout,
    upcat,
    kbuf,
    vbuf,
    xbuf,
    acc,
    rs_out,
    rs_in,
    ag_out,
    estage,
    ebuf,
    xout,
    w_sem,
    d_send,
    d_recv,
    e_send,
    e_recv,
    ea_send,
    x_recv,
    ag_send,
    rs_send,
    rs_recv,
    o_send,
    o_recv,
):
    S, T, Q, L, H, C, W = dims
    M = L // H
    U = Q * H
    groups = xin_ref.shape[1]
    s = lax.axis_index("section")
    t = lax.axis_index("tensor")
    D = C * T
    heads = C // HEAD_DIM
    lane = lax.broadcasted_iota(jnp.int32, (M, LANES), 1)
    long_lane = lax.broadcasted_iota(jnp.int32, (L, LANES), 1)

    def dev(sec, ten):
        return {"section": sec, "tensor": ten}

    def weight_copies():
        cps = [
            pltpu.make_async_copy(wq_hbm, wcat.at[:, pl.ds(LANES, C)], w_sem.at[0]),
            pltpu.make_async_copy(wk_hbm, wcat.at[:, pl.ds(LANES + C, C)], w_sem.at[1]),
            pltpu.make_async_copy(wv_hbm, wcat.at[:, pl.ds(LANES + 2 * C, C)], w_sem.at[2]),
            pltpu.make_async_copy(
                down_hbm,
                wcat.at[pl.ds(pl.multiple_of(t * C, C), C), pl.ds(0, LANES)],
                w_sem.at[3],
            ),
        ]
        for b in range(T):
            cps.append(
                pltpu.make_async_copy(wo_hbm.at[:, pl.ds(b * C, C)], wout.at[b], w_sem.at[4 + b])
            )
        return cps

    for cp in weight_copies():
        cp.start()

    barrier = pltpu.get_barrier_semaphore()

    def greet(i, c):
        sec = i // T
        ten = i % T

        @pl.when(jnp.logical_not(jnp.logical_and(sec == s, ten == t)))
        def _():
            pl.semaphore_signal(barrier, inc=1, device_id=dev(sec, ten), device_id_type=MESH)

        return c

    lax.fori_loop(0, S * T, greet, 0)

    estage[...] = jnp.zeros_like(estage)
    for q in range(Q):
        estage[q, :, 0:W] = xin_ref[entry_ref[q // groups], q % groups]
    kbuf[...] = jnp.zeros_like(kbuf)
    vbuf[...] = jnp.zeros_like(vbuf)
    upcat[...] = jnp.zeros_like(upcat)
    upcat[0 : upcat.shape[0] // 2, 0:C] = up_ref[0]
    upcat[upcat.shape[0] // 2 :, C:] = up_ref[1]
    pl.semaphore_wait(barrier, S * T - 1)

    home = s // 2
    slot = (s % 2) * T + t

    def entry_copy(q):
        return pltpu.make_async_remote_copy(
            src_ref=estage.at[q],
            dst_ref=ebuf.at[slot],
            send_sem=e_send.at[q],
            recv_sem=e_recv.at[slot],
            device_id=dev(q, home),
            device_id_type=MESH,
        )

    def entry_start(q, c):
        mine = jnp.logical_and(q == s, t == home)

        @pl.when(jnp.logical_not(mine))
        def _():
            entry_copy(q).start()

        @pl.when(mine)
        def _():
            ebuf[slot] = estage[q]

        return c

    lax.fori_loop(0, S, entry_start, 0)

    def down_copy(k):
        return pltpu.make_async_remote_copy(
            src_ref=down_hbm,
            dst_ref=wcat.at[pl.ds(pl.multiple_of(t * C, C), C), pl.ds(0, LANES)],
            send_sem=d_send.at[k - 1],
            recv_sem=d_recv.at[k - 1],
            device_id=dev(s, lax.rem(t + k, T)),
            device_id_type=MESH,
        )

    @pl.when(s == 0)
    def _():
        for k in (2, 1, 3):
            down_copy(k).start()

    def entry_wait(i, c):
        src_s = 2 * t + i // T
        src_t = i % T

        @pl.when(jnp.logical_not(jnp.logical_and(src_s == s, src_t == t)))
        def _():
            pltpu.make_async_remote_copy(
                src_ref=estage.at[0],
                dst_ref=ebuf.at[i],
                send_sem=e_send.at[0],
                recv_sem=e_recv.at[i],
                device_id=dev(s, t),
                device_id_type=MESH,
            ).wait_recv()

        return c

    pieces = 2 * T
    lax.fori_loop(0, pieces, entry_wait, 0)
    blocks = [jnp.zeros((L, LANES), F32) for _ in range(C // LANES)]
    for i in range(pieces):
        b, o = divmod(i * W, LANES)
        val = ebuf[i].astype(F32)
        val = jnp.where(long_lane < W, val, 0.0)
        if o:
            val = pltpu.roll(val, o, 1)
        if o + W <= LANES:
            blocks[b] = blocks[b] + val
        else:
            blocks[b] = blocks[b] + jnp.where(long_lane >= o, val, 0.0)
            blocks[b + 1] = blocks[b + 1] + jnp.where(long_lane < o + W - LANES, val, 0.0)
    entered = jnp.concatenate(blocks, axis=1).astype(BF16)

    def entry_spread(h, k):
        return pltpu.make_async_remote_copy(
            src_ref=ag_out.at[U + h],
            dst_ref=xbuf.at[H * s + h, t],
            send_sem=ea_send.at[h, k],
            recv_sem=x_recv.at[H * s + h, t],
            device_id=dev(0, lax.rem(t + k, T)),
            device_id_type=MESH,
        )

    for h in range(H):
        ag_out[U + h] = entered[h * M : (h + 1) * M]
        for k in (2, 1, 3):
            entry_spread(h, k).start()

        @pl.when(s > 0)
        def _():
            entry_spread(h, 0).start()

        @pl.when(s == 0)
        def _():
            xbuf[h, t] = entered[h * M : (h + 1) * M]

    @pl.when(s > 0)
    def _():
        for k in (2, 1, 3):
            down_copy(k).start()

    for cp in weight_copies():
        cp.wait()
    for k in (1, 3, 2):
        down_copy(k).wait_recv()

    row = lax.broadcasted_iota(jnp.int32, (M, L), 0)
    col = lax.broadcasted_iota(jnp.int32, (M, L), 1)
    owner = lax.broadcasted_iota(jnp.int32, (1, LANES), 1) // ADAPTER_RANK % ADAPTER_JOBS

    def rs_copy(q, k):
        other = lax.rem(t + k, T)
        return pltpu.make_async_remote_copy(
            src_ref=rs_out.at[q, k],
            dst_ref=rs_in.at[q, k],
            send_sem=rs_send.at[q, k],
            recv_sem=rs_recv.at[q, k],
            device_id=dev(s, other),
            device_id_type=MESH,
        )

    def ag_copy(q, k):
        return pltpu.make_async_remote_copy(
            src_ref=ag_out.at[q],
            dst_ref=xbuf.at[q, t],
            send_sem=ag_send.at[q, k],
            recv_sem=x_recv.at[q, t],
            device_id=dev(s + 1, lax.rem(t + k, T)),
            device_id_type=MESH,
        )

    def exit_copy(q, i):
        return pltpu.make_async_remote_copy(
            src_ref=xout.at[q, i],
            dst_ref=out_ref.at[q],
            send_sem=o_send.at[q, i],
            recv_sem=o_recv.at[q],
            device_id=dev(2 * t + i // T, i % T),
            device_id_type=MESH,
        )

    def arrive(q, p):
        pltpu.make_async_remote_copy(
            src_ref=ag_out.at[0],
            dst_ref=xbuf.at[q, p],
            send_sem=ag_send.at[0, 0],
            recv_sem=x_recv.at[q, p],
            device_id=dev(s, t),
            device_id_type=MESH,
        ).wait_recv()

    def product(q, ks, ss):
        total = None
        for k in ks:
            p = lax.rem(t + k, T)
            xf = xbuf[q, p].astype(F32)
            sq = xf * xf
            for b in range(C // LANES):
                ss = ss + sq[:, b * LANES : (b + 1) * LANES]
            xg = (xf * gain_ref[p]).astype(BF16)
            prod = jnp.dot(
                xg, wcat[pl.ds(pl.multiple_of(p * C, C), C), :], preferred_element_type=F32
            )
            total = prod if total is None else total + prod
        return total, ss

    def phase_a(q):
        pl.when(jnp.logical_not(jnp.logical_and(s == 0, q < H)))(lambda: arrive(q, t))
        for k in (1, 3):
            arrive(q, lax.rem(t + k, T))
        acc[...], ss = product(q, (0, 1, 3), jnp.zeros((M, LANES), F32))
        far = lax.rem(t + 2, T)
        arrive(q, far)
        xf = xbuf[q, far].astype(F32)
        sq = xf * xf
        for b in range(C // LANES):
            ss = ss + sq[:, b * LANES : (b + 1) * LANES]
        return ss, (xf * gain_ref[far]).astype(BF16), pl.ds(pl.multiple_of(far * C, C), C)

    def phase_b(q, ss, xg, rows):
        code_sum = acc[:, :LANES] + jnp.dot(
            xg, wcat[rows, 0:LANES], preferred_element_type=F32
        )
        r = lax.rsqrt(jnp.sum(ss, axis=1, keepdims=True) * (1.0 / D) + 1e-05)
        seq = q // H
        part = q % H
        job = jobs_ref[seq % groups, entry_ref[seq // groups]]
        codes = jnp.where(owner == job, code_sum * (r * 2.0), 0.0).astype(BF16)
        low = jnp.dot(codes, upcat[...], preferred_element_type=F32)
        here = pl.ds(pl.multiple_of(part * M, M), M)
        full = acc[:, LANES:] + jnp.dot(xg, wcat[rows, LANES:], preferred_element_type=F32)
        kbuf[here, :] = (full[:, C : 2 * C] * r).astype(BF16)
        vbuf[here, :] = (full[:, 2 * C :] * r + low[:, C:]).astype(BF16)
        causal = row + part * M >= col
        mixed = []
        for h in range(heads):
            a, b = h * HEAD_DIM, (h + 1) * HEAD_DIM
            qh = (full[:, a:b] * r + low[:, a:b]).astype(BF16)
            sc = lax.dot_general(
                qh, kbuf[:, a:b], (((1,), (1,)), ((), ())), preferred_element_type=F32
            ) * (HEAD_DIM ** (-0.5))
            sc = jnp.where(causal, sc, -jnp.inf)
            wts = jnp.exp(sc - jnp.max(sc, axis=1, keepdims=True))
            mean = jnp.dot(wts.astype(BF16), vbuf[:, a:b], preferred_element_type=F32)
            mixed.append((mean * (1.0 / jnp.sum(wts, axis=1, keepdims=True))).astype(BF16))
        mix = jnp.concatenate(mixed, axis=1)
        for k in (2, 1, 3, 0):
            other = lax.rem(t + k, T)
            rs_out[q, k] = jnp.dot(mix, wout[other], preferred_element_type=F32).astype(BF16)
        for k in (2, 1, 3):
            rs_copy(q, k).start()

    def phase_c(q):
        total = xbuf[q, t].astype(F32) + rs_out[q, 0].astype(F32)
        for k in (1, 3, 2):
            rs_copy(q, k).wait_recv()
        for k in (1, 3, 2):
            total = total + rs_in[q, k].astype(F32)

        @pl.when(s < S - 1)
        def _():
            ag_out[q] = total.astype(BF16)
            for k in (2, 1, 3, 0):
                ag_copy(q, k).start()

        @pl.when(s == S - 1)
        def _():
            ag_out[q] = total.astype(BF16)
            for i in range(pieces):
                b, o = divmod(i * W, LANES)
                val = total[:, b * LANES : (b + 1) * LANES]
                if o + W > LANES:
                    nxt = total[:, (b + 1) * LANES : (b + 2) * LANES]
                    val = jnp.where(lane >= o, val, nxt)
                if o:
                    val = pltpu.roll(val, LANES - o, 1)
                xout[q, i] = val.astype(BF16)

            for i in range(pieces - 1):
                exit_copy(q, i).start()

            @pl.when(t < T - 1)
            def _():
                exit_copy(q, pieces - 1).start()

            @pl.when(t == T - 1)
            def _():
                out_ref[q] = xout[q, pieces - 1]

    def step(q, c):
        @pl.when(q < U)
        def _():
            phase_b(q, *phase_a(q))

        @pl.when(q > 0)
        def _():
            phase_c(q - 1)

        return c

    lax.fori_loop(0, U + 1, step, 0)

    last = jnp.logical_and(s == S - 1, t == T - 1)

    def finish(q, c):
        @pl.when(jnp.logical_not(last))
        def _():
            pltpu.make_async_remote_copy(
                src_ref=xout.at[q, 0],
                dst_ref=out_ref.at[q],
                send_sem=o_send.at[q, 0],
                recv_sem=o_recv.at[q],
                device_id=dev(s, t),
                device_id_type=MESH,
            ).wait_recv()

        for k in (1, 2, 3):
            rs_copy(q, k).wait_send()

        @pl.when(s < S - 1)
        def _():
            for k in range(T):
                ag_copy(q, k).wait_send()

        @pl.when(s == S - 1)
        def _():
            for i in range(pieces - 1):
                exit_copy(q, i).wait_send()

            @pl.when(t < T - 1)
            def _():
                exit_copy(q, pieces - 1).wait_send()

        return c

    lax.fori_loop(0, U, finish, 0)
    for q in range(S):

        @pl.when(jnp.logical_not(jnp.logical_and(s == q, t == home)))
        def _():
            entry_copy(q).wait_send()

    for k in (1, 2, 3):
        down_copy(k).wait_send()
        for h in range(H):
            entry_spread(h, k).wait_send()

    @pl.when(s > 0)
    def _():
        for h in range(H):
            entry_spread(h, 0).wait_send()


def shards(
    inputs,
    sequence_jobs,
    entry_sequence,
    layer_norm_gain,
    frozen_query_matrix,
    frozen_key_matrix,
    frozen_value_matrix,
    frozen_output_matrix,
    adapter_down_maps,
    adapter_up_maps,
):
    S = lax.axis_size("section")
    T = lax.axis_size("tensor")
    batches, groups, L, W = inputs.shape
    Q = batches * groups
    H = UNITS_PER_SEQUENCE
    U, M = Q * H, L // H
    C = frozen_query_matrix.shape[2]
    D = C * T
    ranks = adapter_down_maps.shape[2]
    jobs = jnp.transpose(sequence_jobs, (1, 2, 0)).reshape(groups, batches)
    gain = layer_norm_gain.reshape(T, 1, C)

    vm = pl.BlockSpec(memory_space=pltpu.VMEM)
    hb = pl.BlockSpec(memory_space=pl.ANY)
    sm = pl.BlockSpec(memory_space=pltpu.SMEM)
    dma = pltpu.SemaphoreType.DMA
    out = pl.pallas_call(
        functools.partial(relay_kernel, (S, T, Q, L, H, C, W)),
        out_shape=jax.ShapeDtypeStruct((U, M, LANES), BF16),
        in_specs=[sm, sm, vm, vm, vm, hb, hb, hb, hb, hb],
        out_specs=vm,
        scratch_shapes=[
            pltpu.VMEM((D, 3 * C + ranks), BF16),
            pltpu.VMEM((T, C, C), BF16),
            pltpu.VMEM((ranks, 2 * C), BF16),
            pltpu.VMEM((L, C), BF16),
            pltpu.VMEM((L, C), BF16),
            pltpu.VMEM((U, T, M, C), BF16),
            pltpu.VMEM((M, 3 * C + ranks), F32),
            pltpu.VMEM((U, T, M, C), BF16),
            pltpu.VMEM((U, T, M, C), BF16),
            pltpu.VMEM((U + H, M, C), BF16),
            pltpu.VMEM((Q, L, LANES), BF16),
            pltpu.VMEM((2 * T, L, LANES), BF16),
            pltpu.VMEM((U, 2 * T, M, LANES), BF16),
            dma((4 + T,)),
            dma((3,)),
            dma((3,)),
            dma((S,)),
            dma((2 * T,)),
            dma((H, T)),
            dma((U, T)),
            dma((U, T)),
            dma((U, T)),
            dma((U, T)),
            dma((U, 2 * T)),
            dma((U,)),
        ],
        compiler_params=pltpu.CompilerParams(
            collective_id=0, has_side_effects=True, vmem_limit_bytes=56 * 1024 * 1024
        ),
        name="relay",
    )(
        entry_sequence,
        jobs,
        inputs,
        gain,
        adapter_up_maps[0],
        adapter_down_maps[0],
        frozen_query_matrix[0],
        frozen_key_matrix[0],
        frozen_value_matrix[0],
        frozen_output_matrix[0],
    )
    return out[:, :, :W].reshape(batches, groups, L, W)


def solution(mesh):
    in_specs = (
        P("dp", None, None, ("section", "tensor")),
        P("dp", None, None),
        P("dp"),
        P("section", None),
        P("section", None, "tensor"),
        P("section", None, "tensor"),
        P("section", None, "tensor"),
        P("section", "tensor", None),
        P("section", "tensor", None),
        P("section", None, None, "tensor"),
    )
    out_specs = P("dp", None, None, ("section", "tensor"))
    return jax.shard_map(shards, mesh=mesh, in_specs=in_specs, out_specs=out_specs, check_vma=False)
```
